32 devices in a mesh: gx: 4 (over y, x), gy: 4 (over z), gz: 2 (over core).
Axes of the slice: x: 2, y: 2, z: 4, core: 2. Of those that a mesh axis runs over, the one named last changes fastest.
Arguments:
- s_blocks: bfloat16 [32, 4, 128, 128], P(('gx', 'gy', 'gz')), may hold values from -1 to 2
- s_columns: int32 [32, 4], P(('gx', 'gy', 'gz')), may hold values from 0 to 6, as said below
- new_home: int32 [32], P(('gx', 'gy', 'gz')), may hold values from 0 to 1, as said below
- z_pattern: int32 [32, 7], P(('gx', 'gy', 'gz')), may hold values 0 or 1
- y_pattern: int32 [32, 7], P(('gx', 'gy', 'gz')), may hold values 0 or 1
Outputs:
- z_out: bfloat16 [32, 128, 7, 128], P(('gx', 'gy', 'gz'))
- y_out: bfloat16 [32, 128, 7, 128], P(('gx', 'gy', 'gz'))
The draws below stay inside these ranges and needn't reach their ends.
Inputs may be any that keep to these rules, and one draw needn't show every extreme that they name: new_home = 1 * (new gz index) + new slot; among the clusters of devices that share gx and gy indices each value occurs once, and the 1 clusters of one device go to 1 different devices. `s_columns`: the entries of a row are distinct, and the first is the cluster's own diagonal block in the new layout (part 0, its new slot).
All inputs are finite; a program needn't handle non-finite values. No bound on the sum of `z_pattern` or of `y_pattern` on one device may be relied on, other than what follows from the above.
Results may differ from the reference program's by a relative error of at most 0.0058.
Values may be sent and summed in bfloat16 or wider, within the bound.
No kernel may reach another device: no remote copies, remote signals or barrier semaphores. Data moves between devices by JAX's collectives and lax.ppermute only.
A program may use at most 64 MiB of HBM per device.

```python
import math
import jax
import jax.numpy as jnp
from jax import lax

B = 128
SLOTS = 1
NB = 4
ITERS = 2
CLUSTERS = 32
N_GX = 4
N_GY = 4
N_GZ = 2


def home_table(key):
    lines = N_GX * N_GY

    def one_line(line_key):
        first, second, third = jax.random.split(line_key, 3)
        shuffle = jax.random.permutation(first, N_GZ)
        offsets = jax.random.permutation(second, N_GZ)[:SLOTS]
        flips = jax.random.randint(third, (N_GZ,), 0, SLOTS)
        source = jnp.arange(N_GZ)[:, None]
        device = shuffle[(source + offsets[None, :]) % N_GZ]
        landing = (jnp.arange(SLOTS)[None, :] + flips[device]) % SLOTS
        return device * SLOTS + landing
    table = jax.vmap(one_line)(jax.random.split(key, lines))
    return table.reshape(-1).astype(jnp.int32)


def draw_new_home(key, part):
    return home_table(jax.random.fold_in(key, 7))


def draw_s_columns(key, part):
    homes = home_table(jax.random.fold_in(key, 7))
    landing = (homes % SLOTS).astype(jnp.int32)
    total = homes.shape[0]

    def one_row(row_key, own):
        picks = jax.random.permutation(row_key, 7 * SLOTS - 1)[:NB - 1].astype(jnp.int32)
        picks = picks + (picks >= own).astype(jnp.int32)
        return jnp.concatenate([own[None], picks])
    row_keys = jax.random.split(jax.random.fold_in(key, 19), total)
    return jax.vmap(one_row)(row_keys, landing).astype(jnp.int32)


def draw_s_blocks(key, part):
    spread = 0.45 / math.sqrt(NB * B)
    first = jax.random.fold_in(jax.random.fold_in(key, 31), 0)
    shape = (CLUSTERS, NB, B, B)
    noise = jax.random.normal(first, shape, jnp.float32)
    values = noise * spread
    values = values.at[:, 0].add(jnp.eye(B, dtype=jnp.float32))
    return values.astype(jnp.bfloat16)


def place_ends(entries, key, low, top_value):
    place = [jax.random.randint(jax.random.fold_in(key, axis), (), 0, length) for axis, length in enumerate(entries.shape)]
    main_axis = entries.shape.index(max(entries.shape))
    neighbour = place[:main_axis] + [(place[main_axis] + 1) % entries.shape[main_axis]] + place[main_axis + 1:]
    return entries.at[tuple(place)].set(low).at[tuple(neighbour)].set(top_value)


def setup_inputs(seed: int = 0) -> dict:
    key_list = jax.random.split(jax.random.key(seed), 6)
    return {
        "s_blocks": draw_s_blocks(jax.random.fold_in(key_list[5], 71), 0),
        "s_columns": draw_s_columns(jax.random.fold_in(key_list[5], 71), 0),
        "new_home": draw_new_home(jax.random.fold_in(key_list[5], 71), 0),
        "z_pattern": place_ends((jax.random.randint(key_list[3], (CLUSTERS, 7 * SLOTS), 0, 3) < 2).astype(jnp.int32), jax.random.fold_in(key_list[3], 1), 0, 1),
        "y_pattern": place_ends((jax.random.randint(key_list[4], (CLUSTERS, 7 * SLOTS), 0, 3) < 2).astype(jnp.int32), jax.random.fold_in(key_list[4], 1), 0, 1),
    }


SHIFTS = ((0, 1, 2), (0, -1, 1), (1, 1, 4), (1, -1, 3), (2, 1, 6), (2, -1, 5))


def neighbour_grid(matrix, axis_pos, offset):
    length = matrix.shape[axis_pos]
    zeros = jnp.zeros_like(lax.slice_in_dim(matrix, 0, 1, axis=axis_pos))
    if offset == 1:
        return jnp.concatenate([zeros, lax.slice_in_dim(matrix, 0, length - 1, axis=axis_pos)], axis=axis_pos)
    return jnp.concatenate([lax.slice_in_dim(matrix, 1, length, axis=axis_pos), zeros], axis=axis_pos)


def halo_grid(matrix):
    pieces = []
    for axis_pos, offset, facing in SHIFTS:
        nearby = neighbour_grid(matrix, axis_pos, offset)
        pieces.append(jnp.stack([nearby[..., :, 0, :], nearby[..., :, facing, :]], axis=-2))
    return jnp.stack(pieces, axis=3)


def block_product(left, right, halo):
    block_size = left.shape[0]
    left_wide = left.astype(jnp.float32)
    right_wide = right.astype(jnp.float32)
    halo_wide = halo.astype(jnp.float32)
    stacked = jnp.concatenate([right_wide[:, 0, :][None], halo_wide[:, :, 1, :]], axis=0).reshape(7 * block_size, block_size)
    own_column = jnp.dot(left_wide.reshape(block_size, 7 * block_size), stacked, precision=lax.Precision.HIGHEST)
    across = jnp.dot(left_wide[:, 0, :], right_wide[:, 1:, :].reshape(block_size, 6 * block_size), precision=lax.Precision.HIGHEST).reshape(block_size, 6, block_size)
    across = across + jnp.einsum("irj,rjk->irk", left_wide[:, 1:, :], halo_wide[:, :, 0, :], precision=lax.Precision.HIGHEST)
    return jnp.concatenate([own_column[:, None, :], across], axis=1)


def grid_product(left, right):
    halo = halo_grid(right)
    result = lax.map(lambda items: block_product(items[0], items[1], items[2]),
                     (left.reshape((-1,) + left.shape[3:]), right.reshape((-1,) + right.shape[3:]), halo.reshape((-1,) + halo.shape[3:])))
    return result.reshape(left.shape[:3] + result.shape[1:])


def masked(retain, matrix):
    shape = matrix.shape
    blocked = matrix.reshape(shape[:3] + (SLOTS, B, 7, SLOTS, B))
    chosen = jnp.where(retain[:, :, :, :, None, :, :, None], blocked, jnp.zeros((), matrix.dtype))
    return chosen.reshape(shape)


def reference(s_blocks, s_columns, new_home, z_pattern, y_pattern):
    lines = N_GX * N_GY
    per_line = N_GZ * SLOTS
    blocks = s_blocks.reshape(lines, per_line, NB, B, B)
    columns = s_columns.reshape(lines, per_line, NB)
    homes = new_home.reshape(lines, per_line).astype(jnp.int32)
    line_ids = jnp.arange(lines, dtype=jnp.int32)[:, None]
    placed = jnp.zeros_like(blocks).at[line_ids, homes].set(blocks)
    placed_cols = jnp.zeros_like(columns).at[line_ids, homes].set(columns)
    slot_ids = jnp.arange(7 * SLOTS, dtype=jnp.int32)
    dense = jnp.zeros((lines, per_line, B, 7 * SLOTS, B), jnp.bfloat16)
    for position in range(NB):
        hits = placed_cols[:, :, position][..., None] == slot_ids
        dense = dense + jnp.where(hits[:, :, None, :, None], placed[:, :, position][:, :, :, None, :], jnp.zeros((), jnp.bfloat16))
    rows_total = SLOTS * B
    start = dense.reshape(N_GX, N_GY, N_GZ, rows_total, 7, rows_total)
    place_x = jnp.arange(N_GX)[:, None, None] + jnp.zeros((N_GX, N_GY, N_GZ), jnp.int32)
    place_y = jnp.arange(N_GY)[None, :, None] + jnp.zeros((N_GX, N_GY, N_GZ), jnp.int32)
    place_z = jnp.arange(N_GZ)[None, None, :] + jnp.zeros((N_GX, N_GY, N_GZ), jnp.int32)
    valid = jnp.stack([place_x >= 0, place_x > 0, place_x < N_GX - 1, place_y > 0, place_y < N_GY - 1,
                       place_z > 0, place_z < N_GZ - 1], axis=-1)
    own_slot = jnp.arange(SLOTS)
    diagonal = (jnp.arange(7)[None, :, None] == 0) & (own_slot[:, None, None] == own_slot[None, None, :])
    shape_keep = (N_GX, N_GY, N_GZ, SLOTS, 7, SLOTS)
    retain_valid = jnp.broadcast_to(valid[:, :, :, None, :, None], shape_keep)
    retain_y = ((y_pattern.reshape(shape_keep) == 1) | diagonal) & valid[:, :, :, None, :, None]
    retain_z = ((z_pattern.reshape(shape_keep) == 1) | diagonal) & valid[:, :, :, None, :, None]
    identity = jnp.concatenate([jnp.eye(rows_total, dtype=jnp.float32)[:, None, :],
                                jnp.zeros((rows_total, 6, rows_total), jnp.float32)], axis=1)
    square = masked(retain_valid, start)
    inverse = jnp.broadcast_to(identity.astype(jnp.bfloat16), start.shape)
    for turn_index in range(ITERS):
        quad = masked(retain_y, grid_product(inverse, square))
        middle = masked(retain_y, 1.5 * identity - 0.5 * quad).astype(jnp.bfloat16)
        square_next = masked(retain_y, grid_product(square, middle)).astype(jnp.bfloat16)
        inverse = masked(retain_z, grid_product(middle, inverse)).astype(jnp.bfloat16)
        square = square_next
    out_shape = (CLUSTERS, B, 7 * SLOTS, B)
    return inverse.reshape(out_shape), square.reshape(out_shape)
```

```python
import functools

import jax
import jax.numpy as jnp
from jax import lax
from jax.experimental import pallas as pl
from jax.experimental.pallas import tpu as pltpu
from jax.sharding import PartitionSpec as P

AXES = ("gx", "gy", "gz")
PARTS = 7
LINKS = ("xa", "xb", "ya", "yb", "z")


def even_partner(i, n):
    j = i ^ 1
    return j if j < n else None


def odd_partner(i, n):
    j = i + 1 if i % 2 else i - 1
    return j if 0 <= j < n else None


def swap_pairs(sizes, link):
    nx, ny, nz = sizes
    pairs = []
    for x in range(nx):
        for y in range(ny):
            for z in range(nz):
                to = None
                if link[0] == "x":
                    near = (even_partner if link == "xa" else odd_partner)(x, nx)
                    to = None if near is None else (near, y, z)
                elif link[0] == "y":
                    near = (even_partner if link == "ya" else odd_partner)(y, ny)
                    to = None if near is None else (x, near, z)
                if to is None:
                    to = (x, y, z ^ 1)
                pairs.append(((x * ny + y) * nz + z, (to[0] * ny + to[1]) * nz + to[2]))
    return pairs


def place(sizes):
    nx, ny, nz = sizes
    x, y, z = (lax.axis_index(a) for a in AXES)
    slots, valids = [], []
    for pos, n, base in ((x, nx, 1), (y, ny, 3)):
        odd = pos % 2
        slots += [base + 1 - odd, base + odd]
        valids += [(odd == 1) | (pos + 1 < n), jnp.where(odd == 1, pos + 1 < n, pos > 0)]
    slots.append(6 - z)
    valids.append(z >= 0)
    return slots, valids


def eye_scaled(size, dtype=jnp.float32):
    rows = lax.broadcasted_iota(jnp.int32, (size, size), 0)
    cols = lax.broadcasted_iota(jnp.int32, (size, size), 1)
    return jnp.where(rows == cols, jnp.asarray(1.5, dtype), jnp.asarray(0.0, dtype))


def keep(flag, block):
    return jnp.where(flag, block, jnp.zeros_like(block))


def mm(a, b):
    return jnp.dot(a, b, preferred_element_type=jnp.float32)


def half(block):
    return (block.astype(jnp.float32) * -0.5).astype(jnp.bfloat16)


def corrected(eye, block):
    return (eye - 0.5 * block.astype(jnp.float32)).astype(jnp.bfloat16)


def place_kernel(sizes, own_cols, other_cols, home, ypat, zpat, own, other, row, *messages):
    count, size = own.shape[1], own.shape[2]
    slots, valids = place(sizes)
    moved = home[0] != lax.axis_index("gz")
    cols = [jnp.where(moved, other_cols[0, k], own_cols[0, k]) for k in range(count)]

    def pick(slot, valid):
        index = jnp.int32(0)
        found = jnp.bool_(False)
        for k in range(count):
            hit = cols[k] == slot
            index = jnp.where(hit, k, index)
            found = found | hit
        block = jnp.where(moved, other[0, index], own[0, index])
        return keep(found & valid, block)

    diag = pick(jnp.int32(0), jnp.bool_(True))
    row[0] = diag
    for q, message in enumerate(messages):
        slot, valid = slots[q], valids[q]
        block = pick(slot, valid)
        row[q + 1] = block
        message[0:size] = diag
        message[size : 2 * size] = keep(ypat[0, slot] == 1, block)
        flag = jnp.where(zpat[0, slot] == 1, 1.0, 0.0)
        message[2 * size :] = jnp.full((message.shape[0] - 2 * size, size), flag, jnp.bfloat16)


def unpack(message, size, valid):
    return message[0:size], keep(valid, message[size : 2 * size])


def diagonal_kernel(sizes, ypat, zpat, row, *refs):
    n = len(LINKS)
    messages, packed, ycol = refs[:n], refs[n], refs[n + 1]
    size = row.shape[1]
    slots, valids = place(sizes)
    eye = eye_scaled(size)
    diag = row[0]
    t0 = corrected(eye, diag)
    total = mm(diag, t0)
    cols = []
    for q in range(n):
        near_diag, facing = unpack(messages[q], size, valids[q])
        tfacing = half(facing)
        total += mm(row[q + 1], tfacing)
        col = (mm(near_diag, tfacing) + mm(facing, t0)).astype(jnp.bfloat16)
        ycol[q] = col
        cols.append(col)
    y0 = total.astype(jnp.bfloat16)
    quad = mm(t0, y0)
    for q in range(n):
        both = (ypat[0, slots[q]] == 1) & (zpat[0, slots[q]] == 1)
        quad += mm(half(keep(both, row[q + 1])), cols[q])
    packed[0:size] = y0
    packed[size:] = (eye - 0.5 * quad).astype(jnp.bfloat16)


def between_kernel(sizes, ypat, row, packed, ycol, *refs):
    n = len(LINKS)
    messages, yrow, yown = refs[:n], refs[n], refs[n + 1]
    size = row.shape[1]
    slots, valids = place(sizes)
    eye = eye_scaled(size)
    diag, y0, tm0 = row[0], packed[0:size], packed[size:]
    total = mm(y0, tm0)
    for q in range(n):
        near_diag, facing = unpack(messages[q], size, valids[q])
        near_t = corrected(eye, near_diag)
        kept = ypat[0, slots[q]] == 1
        block = row[q + 1]
        y1 = keep(kept, (mm(diag, half(block)) + mm(block, near_t)).astype(jnp.bfloat16))
        yrow[q] = y1
        zflag = messages[q][2 * size : 2 * size + 1, 0:1] > 0
        zfacing = jnp.where(zflag, half(facing), jnp.zeros_like(facing))
        quad = mm(near_t, ycol[q]) + mm(zfacing, y0)
        total += mm(y1, (-0.5 * quad).astype(jnp.bfloat16))
    yown[...] = total.astype(jnp.bfloat16)


def last_kernel(sizes, ypat, zpat, row, packed, yrow, yown, *refs):
    n = len(LINKS)
    messages, arrived, zout, yout = refs[:n], refs[n : 2 * n], refs[2 * n], refs[2 * n + 1]
    size = row.shape[1]
    slots, valids = place(sizes)
    eye = eye_scaled(size)
    y0, tm0 = packed[0:size], packed[size:]
    t0 = corrected(eye, row[0])
    total = mm(tm0, t0)
    for q in range(n):
        slot = slots[q]
        kept_y = ypat[0, slot] == 1
        kept_z = zpat[0, slot] == 1
        near_diag, facing = unpack(messages[q], size, valids[q])
        near_t = corrected(eye, near_diag)
        near_y, near_tm = arrived[q][0:size], arrived[q][size:]
        zrow = half(keep(kept_y & kept_z, row[q + 1]))
        y1 = yrow[q]
        quad = mm(t0, y1) + mm(zrow, near_y)
        tm = keep(kept_y & valids[q], (-0.5 * quad).astype(jnp.bfloat16))
        yout[slot] = keep(
            kept_y & valids[q], (mm(y0, tm) + mm(y1, near_tm)).astype(jnp.bfloat16)
        )
        zout[slot] = keep(
            kept_z & valids[q], (mm(tm0, zrow) + mm(tm, near_t)).astype(jnp.bfloat16)
        )
        zflag = messages[q][2 * size : 2 * size + 1, 0:1] > 0
        total += mm(tm, jnp.where(zflag, half(facing), jnp.zeros_like(facing)))
    absent = 11 - slots[-1]
    zout[absent] = jnp.zeros((size, size), jnp.bfloat16)
    yout[absent] = jnp.zeros((size, size), jnp.bfloat16)
    zout[0] = total.astype(jnp.bfloat16)
    yout[0] = yown[...]


def call(kernel, out_shapes, smem, vmem):
    vspec = pl.BlockSpec(memory_space=pltpu.VMEM)
    return pl.pallas_call(
        kernel,
        out_shape=[jax.ShapeDtypeStruct(s, jnp.bfloat16) for s in out_shapes],
        in_specs=[pl.BlockSpec(memory_space=pltpu.SMEM)] * len(smem) + [vspec] * len(vmem),
        out_specs=[vspec] * len(out_shapes),
    )(*smem, *vmem)


def body(sizes, s_blocks, s_columns, new_home, z_pattern, y_pattern):
    size = s_blocks.shape[2]
    n = len(LINKS)
    pairs = {link: swap_pairs(sizes, link) for link in LINKS}

    def send(x, link):
        return lax.ppermute(x, AXES, pairs[link])

    other = send(s_blocks, "z")
    other_cols = send(s_columns, "z")
    row, *messages = call(
        functools.partial(place_kernel, sizes),
        [(n + 1, size, size)] + [(2 * size + 16, size)] * n,
        [s_columns, other_cols, new_home, y_pattern, z_pattern],
        [s_blocks, other],
    )
    messages = [send(m, link) for m, link in zip(messages, LINKS)]
    packed, ycol = call(
        functools.partial(diagonal_kernel, sizes),
        [(2 * size, size), (n, size, size)],
        [y_pattern, z_pattern],
        [row, *messages],
    )
    arrived = [send(packed, link) for link in LINKS]
    yrow, yown = call(
        functools.partial(between_kernel, sizes),
        [(n, size, size), (size, size)],
        [y_pattern],
        [row, packed, ycol, *messages],
    )
    zout, yout = call(
        functools.partial(last_kernel, sizes),
        [(PARTS, size, size)] * 2,
        [y_pattern, z_pattern],
        [row, packed, yrow, yown, *messages, *arrived],
    )
    return tuple(jnp.transpose(o, (1, 0, 2))[None] for o in (zout, yout))


def solution(mesh):
    sizes = tuple(mesh.shape[a] for a in AXES)
    in_specs = (
        P(AXES, None, None, None),
        P(AXES, None),
        P(AXES),
        P(AXES, None),
        P(AXES, None),
    )
    out_specs = (P(AXES, None, None, None), P(AXES, None, None, None))
    return jax.shard_map(
        functools.partial(body, sizes),
        mesh=mesh,
        in_specs=in_specs,
        out_specs=out_specs,
        check_vma=False,
    )
```

```python
import functools

import jax
import jax.numpy as jnp
from jax import lax
from jax.experimental import pallas as pl
from jax.experimental.pallas import tpu as pltpu
from jax.sharding import PartitionSpec as P

AXES = ("gx", "gy", "gz")
PARTS = 7
LINKS = ("xa", "xb", "ya", "yb", "z")


def even_partner(i, n):
    j = i ^ 1
    return j if j < n else None


def odd_partner(i, n):
    j = i + 1 if i % 2 else i - 1
    return j if 0 <= j < n else None


def swap_pairs(sizes, link):
    nx, ny, nz = sizes
    pairs = []
    for x in range(nx):
        for y in range(ny):
            for z in range(nz):
                to = None
                if link[0] == "x":
                    near = (even_partner if link == "xa" else odd_partner)(x, nx)
                    to = None if near is None else (near, y, z)
                elif link[0] == "y":
                    near = (even_partner if link == "ya" else odd_partner)(y, ny)
                    to = None if near is None else (x, near, z)
                if to is None:
                    to = (x, y, z ^ 1)
                pairs.append(((x * ny + y) * nz + z, (to[0] * ny + to[1]) * nz + to[2]))
    return pairs


def place(sizes):
    nx, ny, nz = sizes
    x, y, z = (lax.axis_index(a) for a in AXES)
    slots, valids = [], []
    for pos, n, base in ((x, nx, 1), (y, ny, 3)):
        odd = pos % 2
        slots += [base + 1 - odd, base + odd]
        valids += [(odd == 1) | (pos + 1 < n), jnp.where(odd == 1, pos + 1 < n, pos > 0)]
    slots.append(6 - z)
    valids.append(z >= 0)
    return slots, valids


def eye_scaled(size, dtype=jnp.float32):
    rows = lax.broadcasted_iota(jnp.int32, (size, size), 0)
    cols = lax.broadcasted_iota(jnp.int32, (size, size), 1)
    return jnp.where(rows == cols, jnp.asarray(1.5, dtype), jnp.asarray(0.0, dtype))


def keep(flag, block):
    return jnp.where(flag, block, jnp.zeros_like(block))


def mm(a, b):
    return jnp.dot(a, b, preferred_element_type=jnp.float32)


def half(block):
    return (block.astype(jnp.float32) * -0.5).astype(jnp.bfloat16)


def corrected(eye, block):
    return (eye - 0.5 * block.astype(jnp.float32)).astype(jnp.bfloat16)


def place_kernel(sizes, own_cols, other_cols, home, ypat, zpat, own, other, flags, row, *messages):
    count, size = own.shape[1], own.shape[2]
    n = len(LINKS)
    slots, valids = place(sizes)
    moved = home[0] != lax.axis_index("gz")
    cols = [jnp.where(moved, other_cols[0, k], own_cols[0, k]) for k in range(count)]

    def pick(slot, valid):
        index = jnp.int32(0)
        found = jnp.bool_(False)
        for k in range(count):
            hit = cols[k] == slot
            index = jnp.where(hit, k, index)
            found = found | hit
        block = jnp.where(moved, other[0, index], own[0, index])
        return keep(found & valid, block)

    diag = pick(jnp.int32(0), jnp.bool_(True))
    row[0] = diag
    for q, message in enumerate(messages):
        slot, valid = slots[q], valids[q]
        kept_y = (ypat[0, slot] == 1) & valid
        kept_z = (zpat[0, slot] == 1) & valid
        flags[q] = jnp.where(kept_y, 1, 0)
        flags[n + q] = jnp.where(kept_z, 1, 0)
        block = pick(slot, valid)
        row[q + 1] = block
        message[0:size] = diag
        message[size : 2 * size] = keep(kept_y, block)
        message[2 * size :] = jnp.full(
            (message.shape[0] - 2 * size, size), jnp.where(kept_z, 1.0, 0.0), jnp.bfloat16
        )


def unpack(message, size, valid):
    return message[0:size], keep(valid, message[size : 2 * size])


def diagonal_kernel(sizes, flags, row, *refs):
    n = len(LINKS)
    messages, packed, ycol = refs[:n], refs[n], refs[n + 1]
    size = row.shape[1]
    _, valids = place(sizes)
    eye = eye_scaled(size)
    diag = row[0]
    t0 = corrected(eye, diag)
    total = mm(diag, t0)
    cols = []
    for q in range(n):
        near_diag, facing = unpack(messages[q], size, valids[q])
        tfacing = half(facing)
        total += mm(row[q + 1], tfacing)
        col = (mm(near_diag, tfacing) + mm(facing, t0)).astype(jnp.bfloat16)
        ycol[q] = col
        cols.append(col)
    y0 = total.astype(jnp.bfloat16)
    quad = mm(t0, y0)
    for q in range(n):
        both = (flags[q] == 1) & (flags[n + q] == 1)
        quad += mm(half(keep(both, row[q + 1])), cols[q])
    packed[0:size] = y0
    packed[size:] = (eye - 0.5 * quad).astype(jnp.bfloat16)


def between_kernel(sizes, flags, row, packed, ycol, *refs):
    n = len(LINKS)
    messages, yrow, yown = refs[:n], refs[n], refs[n + 1]
    size = row.shape[1]
    _, valids = place(sizes)
    eye = eye_scaled(size)
    diag, y0, tm0 = row[0], packed[0:size], packed[size:]
    total = mm(y0, tm0)
    for q in range(n):
        near_diag, facing = unpack(messages[q], size, valids[q])
        near_t = corrected(eye, near_diag)
        block = row[q + 1]
        y1 = keep(flags[q] == 1, (mm(diag, half(block)) + mm(block, near_t)).astype(jnp.bfloat16))
        yrow[q] = y1
        zflag = messages[q][2 * size : 2 * size + 1, 0:1] > 0
        zfacing = jnp.where(zflag, half(facing), jnp.zeros_like(facing))
        quad = mm(near_t, ycol[q]) + mm(zfacing, y0)
        total += mm(y1, (-0.5 * quad).astype(jnp.bfloat16))
    yown[...] = total.astype(jnp.bfloat16)


def last_kernel(sizes, flags, row, packed, yrow, yown, *refs):
    n = len(LINKS)
    messages, arrived, zout, yout = refs[:n], refs[n : 2 * n], refs[2 * n], refs[2 * n + 1]
    size = row.shape[1]
    slots, valids = place(sizes)
    eye = eye_scaled(size)
    y0, tm0 = packed[0:size], packed[size:]
    t0 = corrected(eye, row[0])
    total = mm(tm0, t0)
    for q in range(n):
        slot = slots[q]
        kept_y, kept_z = flags[q] == 1, flags[n + q] == 1
        near_diag, facing = unpack(messages[q], size, valids[q])
        near_t = corrected(eye, near_diag)
        near_y, near_tm = arrived[q][0:size], arrived[q][size:]
        zrow = half(keep(kept_y & kept_z, row[q + 1]))
        y1 = yrow[q]
        quad = mm(t0, y1) + mm(zrow, near_y)
        tm = keep(kept_y, (-0.5 * quad).astype(jnp.bfloat16))
        yout[slot] = keep(kept_y, (mm(y0, tm) + mm(y1, near_tm)).astype(jnp.bfloat16))
        zout[slot] = keep(kept_z, (mm(tm0, zrow) + mm(tm, near_t)).astype(jnp.bfloat16))
        zflag = messages[q][2 * size : 2 * size + 1, 0:1] > 0
        total += mm(tm, jnp.where(zflag, half(facing), jnp.zeros_like(facing)))
    absent = 11 - slots[-1]
    zout[absent] = jnp.zeros((size, size), jnp.bfloat16)
    yout[absent] = jnp.zeros((size, size), jnp.bfloat16)
    zout[0] = total.astype(jnp.bfloat16)
    yout[0] = yown[...]


def chip(*shape):
    return pltpu.VMEM(shape, jnp.bfloat16)


def call(kernel, outs, smem, vmem):
    def spec(array):
        return pl.BlockSpec(memory_space=pltpu.SMEM if array.dtype == jnp.int32 else pltpu.VMEM)

    return pl.pallas_call(
        kernel, out_shape=outs, in_specs=[spec(a) for a in (*smem, *vmem)], out_specs=[spec(o) for o in outs]
    )(*smem, *(pltpu.with_memory_space_constraint(v, pltpu.VMEM) for v in vmem))


def body(sizes, s_blocks, s_columns, new_home, z_pattern, y_pattern):
    size = s_blocks.shape[2]
    n = len(LINKS)
    pairs = {link: swap_pairs(sizes, link) for link in LINKS}

    def send(x, link):
        return lax.ppermute(x, AXES, pairs[link])

    other = send(s_blocks, "z")
    other_cols = send(s_columns, "z")
    flags, row, *messages = call(
        functools.partial(place_kernel, sizes),
        [pltpu.SMEM((2 * n,), jnp.int32), chip(n + 1, size, size)] + [chip(2 * size + 16, size)] * n,
        [s_columns, other_cols, new_home, y_pattern, z_pattern],
        [s_blocks, other],
    )
    flags = pltpu.with_memory_space_constraint(flags, pltpu.SMEM)
    messages = [send(m, link) for m, link in zip(messages, LINKS)]
    packed, ycol = call(
        functools.partial(diagonal_kernel, sizes),
        [chip(2 * size, size), chip(n, size, size)],
        [flags],
        [row, *messages],
    )
    arrived = [send(packed, link) for link in LINKS]
    yrow, yown = call(
        functools.partial(between_kernel, sizes),
        [chip(n, size, size), chip(size, size)],
        [flags],
        [row, packed, ycol, *messages],
    )
    result = jax.ShapeDtypeStruct((PARTS, size, size), jnp.bfloat16)
    zout, yout = call(
        functools.partial(last_kernel, sizes),
        [result, result],
        [flags],
        [row, packed, yrow, yown, *messages, *arrived],
    )
    return tuple(jnp.transpose(o, (1, 0, 2))[None] for o in (zout, yout))


def solution(mesh):
    sizes = tuple(mesh.shape[a] for a in AXES)
    in_specs = (
        P(AXES, None, None, None),
        P(AXES, None),
        P(AXES),
        P(AXES, None),
        P(AXES, None),
    )
    out_specs = (P(AXES, None, None, None), P(AXES, None, None, None))
    return jax.shard_map(
        functools.partial(body, sizes),
        mesh=mesh,
        in_specs=in_specs,
        out_specs=out_specs,
        check_vma=False,
    )
```
